32 devices in a mesh: face: 8 (over z, core), sub: 4 (over y, x).
Axes of the slice: x: 2, y: 2, z: 4, core: 2. Of those that a mesh axis runs over, the one named last changes fastest.
Arguments:
- mesh_latent: bfloat16 [8192, 512], P(('face', 'sub')), may hold values from -6 to 6
- edge_latent: bfloat16 [65536, 512], P(('face', 'sub')), may hold values from -6 to 6
- grid_features: bfloat16 [8192, 384], P(('face', 'sub')), may hold values from -6 to 6
- senders: int32 [65536], P(('face', 'sub')), may hold values from 0 to 383, as said below
- receivers: int32 [65536], P(('face', 'sub')), may hold values from 0 to 255
- send_lists: int32 [32, 4, 32], P(('face', 'sub')), may hold values from -1 to 255, as said below
- link_sources: int32 [16384], P(('face', 'sub')), may hold values from 0 to 255
- link_targets: int32 [16384], P(('face', 'sub')), may hold values from 0 to 255
- node_area: float32 [8192], P(('face', 'sub')), may hold values from 0.25 to 4.5
- grid_weight: bfloat16 [384, 512], P(None, 'sub'), may hold values from -0.3125 to 0.3125
- encode_weight: bfloat16 [1024, 512], P('sub'), may hold values from -0.1875 to 0.1875
- edge_first: bfloat16 [1, 1536, 512], P(None, 'sub'), may hold values from -0.15625 to 0.15625
- edge_second: bfloat16 [1, 512, 512], P(None, 'sub'), may hold values from -0.25 to 0.25
- node_first: bfloat16 [1, 1024, 512], P(None, 'sub'), may hold values from -0.1875 to 0.1875
- node_second: bfloat16 [1, 512, 512], P(None, 'sub'), may hold values from -0.25 to 0.25
Outputs:
- mesh_result: bfloat16 [8192, 512], P(('face', 'sub'))
- edge_result: bfloat16 [65536, 512], P(('face', 'sub'))
- masses: float32 [1, 512], replicated
The draws below stay inside these ranges and needn't reach their ends.
Inputs may be any that keep to these rules, and one draw needn't show every extreme that they name: `send_lists`: entries are the sending partition's own node numbers, or -1 for an unused slot; in every list the used slots come first, hold distinct nodes and number 32 // 2 or more; for every list number some partition uses all 32 slots. `senders`: A value below 256 names one of the partition's own nodes; 256 + d * 32 + k names slot k of the list with number d that the partition receives, and that slot is always a used one.
All inputs are finite; a program needn't handle non-finite values.
Results may differ from the reference program's by a relative error of at most 0.008.
Values may be sent and summed in bfloat16 or wider, within the bound.
A program may use at most 64 MiB of HBM per device.

```python
import jax
import jax.numpy as jnp
from jax import lax

D = 512
GFEAT = 384
NODE_DEV = 256
EDGE_DEV = 2048
GRID_DEV = 256
LINK_DEV = 512
HALO = 32
LAYERS = 1
NODES = 8192
EDGES = 65536
GRIDS = 8192
LINKS = 16384
N_FACE = 8
N_SUB = 4


def halo_live(key):
    partitions = N_FACE * N_SUB
    first_key, second_key = jax.random.split(jax.random.fold_in(key, 11))
    live_count = jax.random.randint(first_key, (partitions, 4), HALO // 2, HALO + 1)
    full_device = jax.random.randint(second_key, (4,), 0, partitions)
    live_count = jnp.where(jnp.arange(partitions)[:, None] == full_device[None, :], HALO, live_count)
    return live_count.astype(jnp.int32)


def draw_send_lists(key, part):
    partitions = N_FACE * N_SUB
    live_count = halo_live(key)
    scores = jax.random.randint(jax.random.fold_in(key, 12), (partitions, 4, NODE_DEV), 0, 1 << 20)
    scores = scores * NODE_DEV + jnp.arange(NODE_DEV, dtype=jnp.int32)[None, None, :]
    ranking = jnp.argsort(scores, axis=-1).astype(jnp.int32)[:, :, :HALO]
    slot_index = jnp.arange(HALO, dtype=jnp.int32)
    return jnp.where(slot_index[None, None, :] < live_count[:, :, None], ranking, -1).astype(jnp.int32)


def draw_senders(key, part):
    partitions = N_FACE * N_SUB
    live_count = halo_live(key)
    first_key, second_key, third_key, fourth_key = jax.random.split(jax.random.fold_in(key, 13), 4)
    total = partitions * EDGE_DEV
    device_of = jnp.arange(total, dtype=jnp.int32) // EDGE_DEV
    face_index = device_of // N_SUB
    sub_index = device_of % N_SUB
    direction = jax.random.randint(first_key, (total,), 0, 4)
    source = jnp.where(direction == 0, (face_index - 1) % N_FACE * N_SUB + sub_index, jnp.where(direction == 1, (face_index + 1) % N_FACE * N_SUB + sub_index, jnp.where(direction == 2, face_index * N_SUB + (sub_index - 1) % N_SUB, face_index * N_SUB + (sub_index + 1) % N_SUB)))
    live_here = live_count[source, direction]
    slot_index = jax.random.randint(second_key, (total,), 0, 1 << 20) % live_here
    remote = NODE_DEV + direction * HALO + slot_index
    local_node = jax.random.randint(third_key, (total,), 0, NODE_DEV)
    use_halo = jax.random.randint(fourth_key, (total,), 0, 4) == 0
    return jnp.where(use_halo, remote, local_node).astype(jnp.int32)


def draw_node_area(key, part):
    ramp_scale = 1.0 + 2.0 * jnp.arange(NODES, dtype=jnp.float32) / NODES
    factor = jax.random.uniform(key, (NODES,), jnp.float32, 0.5, 1.5)
    return (ramp_scale * factor).astype(jnp.float32)


def place_ends(drawn, stream_key, low, high):
    index_at = [jax.random.randint(jax.random.fold_in(stream_key, axis), (), 0, length) for axis, length in enumerate(drawn.shape)]
    main_axis = drawn.shape.index(max(drawn.shape))
    neighbour = index_at[:main_axis] + [(index_at[main_axis] + 1) % drawn.shape[main_axis]] + index_at[main_axis + 1:]
    return drawn.at[tuple(index_at)].set(low).at[tuple(neighbour)].set(high)


def shard_levels(key, extent, cuts, smallest, largest):
    def one(axis_at, parts):
        draws = jax.random.uniform(jax.random.fold_in(jax.random.fold_in(key, 6), axis_at), (parts,), jnp.float32, smallest / len(cuts), largest / len(cuts))
        return jnp.repeat(jnp.exp(draws), extent[axis_at] // parts).reshape((-1,) + (1,) * (len(extent) - axis_at - 1))

    factor_of = one(*cuts[0])
    for cut in cuts[1:]:
        factor_of = factor_of * one(*cut)
    return factor_of


def centred(own_key, shape, deviation, limit, cuts=(), kind=jnp.bfloat16):
    gain = shard_levels(own_key, shape, cuts, -0.22, 0.18) if cuts else 1.0
    result = jax.random.normal(own_key, shape, jnp.float32) * deviation * gain
    return jnp.minimum(jnp.maximum(result, -limit), limit).astype(kind)


def setup_inputs(seed: int = 0) -> dict:
    key_of = jax.random.split(jax.random.key(seed), 16)
    return {
        "mesh_latent": centred(key_of[0], (NODES, D), 1.0, 6.0, ((0, 32),)),
        "edge_latent": centred(key_of[1], (EDGES, D), 1.0, 6.0, ((0, 32),)),
        "grid_features": centred(key_of[2], (GRIDS, GFEAT), 1.0, 6.0, ((0, 32),)),
        "senders": draw_senders(jax.random.fold_in(key_of[15], 71), 0),
        "receivers": place_ends(jax.random.randint(key_of[4], (EDGES,), 0, NODE_DEV), jax.random.fold_in(key_of[4], 1), 0, NODE_DEV - 1).astype(jnp.int32),
        "send_lists": draw_send_lists(jax.random.fold_in(key_of[15], 71), 0),
        "link_sources": place_ends(jax.random.randint(key_of[6], (LINKS,), 0, GRID_DEV), jax.random.fold_in(key_of[6], 1), 0, GRID_DEV - 1).astype(jnp.int32),
        "link_targets": place_ends(jax.random.randint(key_of[7], (LINKS,), 0, NODE_DEV), jax.random.fold_in(key_of[7], 1), 0, NODE_DEV - 1).astype(jnp.int32),
        "node_area": draw_node_area(jax.random.fold_in(key_of[15], 71), 0),
        "grid_weight": centred(key_of[9], (GFEAT, D), GFEAT ** -0.5, 0.3125, ((1, 4),)),
        "encode_weight": centred(key_of[10], (2 * D, D), (2 * D) ** -0.5, 0.1875, ((0, 4),)),
        "edge_first": centred(key_of[11], (LAYERS, 3 * D, D), (3 * D) ** -0.5, 0.15625, ((1, 4),)),
        "edge_second": centred(key_of[12], (LAYERS, D, D), D ** -0.5, 0.25, ((1, 4),)),
        "node_first": centred(key_of[13], (LAYERS, 2 * D, D), (2 * D) ** -0.5, 0.1875, ((1, 4),)),
        "node_second": centred(key_of[14], (LAYERS, D, D), D ** -0.5, 0.25, ((1, 4),)),
    }


def global_slots(send_lists):
    partitions = N_FACE * N_SUB
    part_ids = jnp.arange(partitions, dtype=jnp.int32)
    face_index = part_ids // N_SUB
    sub_index = part_ids % N_SUB
    sources = jnp.stack([((face_index - 1) % N_FACE) * N_SUB + sub_index,
                         ((face_index + 1) % N_FACE) * N_SUB + sub_index,
                         face_index * N_SUB + (sub_index - 1) % N_SUB,
                         face_index * N_SUB + (sub_index + 1) % N_SUB], axis=1).astype(jnp.int32)
    incoming_lists = send_lists[sources, jnp.arange(4, dtype=jnp.int32)[None, :], :]
    remote = jnp.where(incoming_lists >= 0, sources[:, :, None] * NODE_DEV + incoming_lists, NODES)
    own_rows = part_ids[:, None] * NODE_DEV + jnp.arange(NODE_DEV, dtype=jnp.int32)[None, :]
    return jnp.concatenate([own_rows, remote.reshape(partitions, 4 * HALO).astype(jnp.int32)], axis=1).astype(jnp.int32)


def reference(mesh_latent, edge_latent, grid_features, senders, receivers, send_lists, link_sources, link_targets, node_area, grid_weight, encode_weight, edge_first, edge_second, node_first, node_second):
    partitions = N_FACE * N_SUB
    grid_latent = jax.nn.silu(jnp.dot(grid_features, grid_weight, preferred_element_type=jnp.float32)).astype(jnp.bfloat16)

    def encode_block(block):
        grid_rows, node_rows, sources, targets = block
        joined = jnp.concatenate([jnp.take(grid_rows, sources, axis=0), jnp.take(node_rows, targets, axis=0)], axis=1)
        messages = jax.nn.silu(jnp.dot(joined, encode_weight, preferred_element_type=jnp.float32)).astype(jnp.bfloat16)
        return jax.ops.segment_sum(messages.astype(jnp.float32), targets, num_segments=NODE_DEV)

    gathered = lax.map(encode_block, (grid_latent.reshape(partitions, GRID_DEV, D),
                                      mesh_latent.reshape(partitions, NODE_DEV, D),
                                      link_sources.reshape(partitions, LINK_DEV),
                                      link_targets.reshape(partitions, LINK_DEV)))
    latent = (mesh_latent.astype(jnp.float32) + gathered.reshape(NODES, D)).astype(jnp.bfloat16)

    slot_table = global_slots(send_lists)
    offsets = (jnp.arange(partitions, dtype=jnp.int32) * NODE_DEV)[:, None]
    local_receivers = receivers.reshape(partitions, EDGE_DEV)
    global_receivers = (local_receivers + offsets).astype(jnp.int32)
    edge_senders = senders.reshape(partitions, EDGE_DEV)
    edge_state = edge_latent.reshape(partitions, EDGE_DEV, D)
    totals = []
    for layer_index in range(LAYERS):
        padded = jnp.concatenate([latent, jnp.zeros((1, D), jnp.bfloat16)], axis=0)
        first_weight = edge_first[layer_index]
        second_weight = edge_second[layer_index]

        def edge_block(block):
            edges, slots, sends, global_recv, local_recv = block
            joined = jnp.concatenate([edges, jnp.take(padded, jnp.take(slots, sends), axis=0),
                                      jnp.take(latent, global_recv, axis=0)], axis=1)
            hidden = jax.nn.silu(jnp.dot(joined, first_weight, preferred_element_type=jnp.float32)).astype(jnp.bfloat16)
            updated = (edges.astype(jnp.float32) + jnp.dot(hidden, second_weight, preferred_element_type=jnp.float32)).astype(jnp.bfloat16)
            incoming = jax.ops.segment_sum(updated.astype(jnp.float32), local_recv, num_segments=NODE_DEV)
            return updated, incoming

        edge_state, incoming = lax.map(edge_block, (edge_state, slot_table, edge_senders, global_receivers, local_receivers))
        incoming = incoming.reshape(NODES, D).astype(jnp.bfloat16)
        node_hidden = jax.nn.silu(jnp.dot(jnp.concatenate([latent, incoming], axis=1), node_first[layer_index],
                                          preferred_element_type=jnp.float32)).astype(jnp.bfloat16)
        latent = (latent.astype(jnp.float32) + jnp.dot(node_hidden, node_second[layer_index],
                                                       preferred_element_type=jnp.float32)).astype(jnp.bfloat16)
        totals.append(jnp.dot(node_area, latent.astype(jnp.float32), precision=lax.Precision.HIGHEST))
    masses = jnp.stack(totals) / NODES
    return latent, edge_state.reshape(EDGES, D), masses
```

```python
import functools

import jax
import jax.numpy as jnp
from jax import lax
from jax.experimental import pallas as pl
from jax.experimental.pallas import tpu as pltpu
from jax.sharding import PartitionSpec as P

MESH = pl.DeviceIdType.MESH
CHUNK = 256
BF = jnp.bfloat16
F32 = jnp.float32


def silu(v):
    return v / (1.0 + jnp.exp(-v))


def mm(a, b):
    return jnp.dot(a, b, preferred_element_type=F32)


def mm_t(a, b):
    return lax.dot_general(a, b, (((0,), (0,)), ((), ())), preferred_element_type=F32)


def hot(rows, index):
    ids = lax.broadcasted_iota(jnp.int32, (rows, index.shape[1]), 0)
    return jnp.where(ids == index, 1.0, 0.0).astype(BF)


def kernel(
    n_face, n_sub,
    mesh_ref, edge_hbm, grid_ref, send_ref, recv_ref, lists_ref, src_ref, dst_ref, area_ref,
    wg, we, w1, w2, v1, v2,
    lat_out, edge_hbm_out, mass_out,
    gg, ge, g1, g2, h1, h2,
    edges, picks, back, table, proj, halo, sums_a, sums_b, total,
    s1, r1, s2, r2, hs, hr, as_, ar, bs, br, ein, eout,
):
    face, sub = lax.axis_index("face"), lax.axis_index("sub")
    core = lax.rem(face, 2)
    partner = face + 1 - 2 * core
    nodes, width = mesh_ref.shape
    chunks = edges.shape[0] // CHUNK

    def load_edges(i):
        rows = pl.ds(pl.multiple_of(i * CHUNK, CHUNK), CHUNK)
        return pltpu.make_async_copy(edge_hbm.at[rows], edges.at[rows], ein.at[i])

    def store_edges(i):
        rows = pl.ds(pl.multiple_of(i * CHUNK, CHUNK), CHUNK)
        return pltpu.make_async_copy(edges.at[rows], edge_hbm_out.at[rows], eout.at[i])

    for i in range(chunks):
        load_edges(i).start()

    barrier = pltpu.get_barrier_semaphore()
    for k in range(1, n_sub):
        pl.semaphore_signal(barrier, inc=1, device_id=(face, lax.rem(sub + k, n_sub)), device_id_type=MESH)
    for k in range(1, n_face):
        pl.semaphore_signal(barrier, inc=1, device_id=(lax.rem(face + k, n_face), sub), device_id_type=MESH)
    pl.semaphore_wait(barrier, n_sub + n_face - 2)

    shards = [wg, we, w1.at[0], w2.at[0], v1.at[0], v2.at[0]]
    wholes = [gg, ge, g1, g2, h1, h2]

    def half_of(w, owner):
        rows = shards[w].shape[0]
        half = rows // 2
        if w == 0:
            return gg.at[owner, pl.ds(pl.multiple_of(core * half, half), half)]
        return wholes[w].at[pl.ds(pl.multiple_of(owner * rows + core * half, half), half)]

    def outward(w, k):
        half = shards[w].shape[0] // 2
        return pltpu.make_async_remote_copy(
            src_ref=shards[w].at[pl.ds(pl.multiple_of(core * half, half), half)],
            dst_ref=half_of(w, sub),
            send_sem=s1.at[w, k], recv_sem=r1.at[w, k],
            device_id=(face, lax.rem(sub + k, n_sub)), device_id_type=MESH)

    def across(w, k):
        part = half_of(w, lax.rem(sub + n_sub - k, n_sub))
        return pltpu.make_async_remote_copy(
            src_ref=part, dst_ref=part, send_sem=s2.at[w, k], recv_sem=r2.at[w, k],
            device_id=(partner, sub), device_id_type=MESH)

    for w in range(6):
        for k in range(1, n_sub):
            outward(w, k).start()

    def pass_on(w):
        for k in range(1, n_sub):
            outward(w, k).wait_recv()
            across(w, k).start()

    def arrive(w):
        for k in range(1, n_sub):
            across(w, k).wait_recv()

    gg[sub] = wg[...]
    for w in range(1, 6):
        rows = shards[w].shape[0]
        wholes[w][pl.ds(pl.multiple_of(sub * rows, rows), rows), :] = shards[w][...]
    slots = nodes + 4 * halo.shape[1]

    def mark(i, carry):
        cols = pl.ds(pl.multiple_of(i * CHUNK, CHUNK), CHUNK)
        here = hot(nodes, recv_ref[:, cols])
        back[:, cols] = here
        both = jnp.concatenate([hot(slots, send_ref[:, cols]), here], axis=0)
        picks[cols, :] = both.T
        return carry

    lax.fori_loop(0, chunks, mark, 0)
    to_node = hot(nodes, dst_ref[...])
    link_pick = jnp.concatenate([hot(grid_ref.shape[0], src_ref[...]), to_node], axis=0)

    pass_on(0)
    arrive(0)
    grid = jnp.concatenate([mm(grid_ref[...], gg[j]) for j in range(n_sub)], axis=1)
    grid = silu(grid).astype(BF)
    pass_on(1)
    arrive(1)
    rows = grid_ref.shape[0]
    from_grid = mm(grid, ge[:width, :]).astype(BF)
    from_mesh = mm(mesh_ref[...], ge[width:, :]).astype(BF)
    message = silu(mm_t(link_pick, jnp.concatenate([from_grid, from_mesh], axis=0))).astype(BF)
    latent = (mesh_ref[...].astype(F32) + mm(to_node, message)).astype(BF)
    table[...] = latent

    size = halo.shape[1]
    for d in range(4):
        halo[d] = mm_t(hot(nodes, lists_ref[0, d:d + 1, :]), latent).astype(BF)

    def border(d):
        step = (1, n_face - 1, 1, n_sub - 1)[d]
        to = (lax.rem(face + step, n_face), sub) if d < 2 else (face, lax.rem(sub + step, n_sub))
        return pltpu.make_async_remote_copy(
            src_ref=halo.at[d], dst_ref=halo.at[4 + d], send_sem=hs.at[d], recv_sem=hr.at[d],
            device_id=to, device_id_type=MESH)

    for d in range(4):
        border(d).start()

    pass_on(2)
    arrive(2)
    proj[:nodes, :] = mm(latent, g1[width:2 * width, :]).astype(BF)
    proj[slots:, :] = mm(latent, g1[2 * width:, :]).astype(BF)
    for d in range(4):
        border(d).wait_recv()
    outer = jnp.concatenate([halo[4 + d] for d in range(4)], axis=0)
    proj[nodes:slots, :] = mm(outer, g1[width:2 * width, :]).astype(BF)
    pass_on(3)
    arrive(3)

    total[...] = jnp.zeros_like(total)
    for i in range(chunks):
        load_edges(i).wait()

    def update(i, carry):
        cols = pl.ds(pl.multiple_of(i * CHUNK, CHUNK), CHUNK)
        edge = edges[cols, :]
        before = mm(edge, g1[:width, :]) + mm(picks[cols, :], proj[...])
        hidden = silu(before).astype(BF)
        new = (edge.astype(F32) + mm(hidden, g2[...])).astype(BF)
        edges[cols, :] = new
        total[...] += mm(back[:, cols], new)
        return carry

    lax.fori_loop(0, chunks // 2, update, 0)
    pass_on(4)
    lax.fori_loop(chunks // 2, chunks, update, 0)
    pass_on(5)
    for i in range(chunks):
        store_edges(i).start()
    arrive(4)
    incoming = total[...].astype(BF)
    hidden = silu(mm(table[...], h1[:width, :]) + mm(incoming, h1[width:, :])).astype(BF)
    arrive(5)
    final = (table[...].astype(F32) + mm(hidden, h2[...])).astype(BF)
    lat_out[...] = final
    part = jnp.dot(area_ref[...], final.astype(F32), precision=lax.Precision.HIGHEST, preferred_element_type=F32)

    def share_sub(k):
        return pltpu.make_async_remote_copy(
            src_ref=sums_a.at[sub], dst_ref=sums_a.at[sub], send_sem=as_.at[k], recv_sem=ar.at[k],
            device_id=(face, lax.rem(sub + k, n_sub)), device_id_type=MESH)

    def share_face(k):
        return pltpu.make_async_remote_copy(
            src_ref=sums_b.at[face], dst_ref=sums_b.at[face], send_sem=bs.at[k], recv_sem=br.at[k],
            device_id=(lax.rem(face + k, n_face), sub), device_id_type=MESH)

    sums_a[sub] = part
    for k in range(1, n_sub):
        share_sub(k).start()
    for k in range(1, n_sub):
        share_sub(k).wait_recv()
    sums_b[face] = jnp.sum(sums_a[...], axis=0)
    for k in range(1, n_face):
        share_face(k).start()
    for k in range(1, n_face):
        share_face(k).wait_recv()
    mass_out[...] = jnp.sum(sums_b[...], axis=0) / (nodes * n_face * n_sub)

    for w in range(6):
        for k in range(1, n_sub):
            outward(w, k).wait_send()
            across(w, k).wait_send()
    for d in range(4):
        border(d).wait_send()
    for k in range(1, n_sub):
        share_sub(k).wait_send()
    for k in range(1, n_face):
        share_face(k).wait_send()
    for i in range(chunks):
        store_edges(i).wait()


def per_device(
    mesh_latent, edge_latent, grid_features, senders, receivers, send_lists, link_sources,
    link_targets, node_area, grid_weight, encode_weight, edge_first, edge_second, node_first,
    node_second,
):
    n_face, n_sub = lax.axis_size("face"), lax.axis_size("sub")
    nodes, width = mesh_latent.shape
    count = edge_latent.shape[0]
    size = send_lists.shape[2]
    slots = nodes + 4 * size
    chunks = count // CHUNK
    dma = pltpu.SemaphoreType.DMA
    vmem = pl.BlockSpec(memory_space=pltpu.VMEM)
    hbm = pl.BlockSpec(memory_space=pl.ANY)
    whole = [pltpu.VMEM((n_sub * w.shape[-2], width), BF)
             for w in (encode_weight, edge_first, edge_second, node_first, node_second)]
    return pl.pallas_call(
        functools.partial(kernel, n_face, n_sub),
        out_shape=(
            jax.ShapeDtypeStruct(mesh_latent.shape, BF),
            jax.ShapeDtypeStruct(edge_latent.shape, BF),
            jax.ShapeDtypeStruct((1, width), F32),
        ),
        in_specs=[vmem, hbm] + [vmem] * 13,
        out_specs=(vmem, hbm, vmem),
        scratch_shapes=[
            pltpu.VMEM((n_sub,) + grid_weight.shape, BF), *whole,
            pltpu.VMEM(edge_latent.shape, BF),
            pltpu.VMEM((count, slots + nodes), BF),
            pltpu.VMEM((nodes, count), BF),
            pltpu.VMEM((nodes, width), BF),
            pltpu.VMEM((slots + nodes, width), BF),
            pltpu.VMEM((8, size, width), BF),
            pltpu.VMEM((n_sub, 1, width), F32),
            pltpu.VMEM((n_face, 1, width), F32),
            pltpu.VMEM((nodes, width), F32),
            dma((6, n_sub)), dma((6, n_sub)), dma((6, n_sub)), dma((6, n_sub)),
            dma((4,)), dma((4,)), dma((n_sub,)), dma((n_sub,)), dma((n_face,)), dma((n_face,)),
            dma((chunks,)), dma((chunks,)),
        ],
        compiler_params=pltpu.CompilerParams(
            collective_id=0, has_side_effects=True, vmem_limit_bytes=48 * 1024 * 1024
        ),
    )(
        mesh_latent, edge_latent, grid_features, senders.reshape(1, -1), receivers.reshape(1, -1),
        send_lists, link_sources.reshape(1, -1), link_targets.reshape(1, -1),
        node_area.reshape(1, -1), grid_weight, encode_weight, edge_first, edge_second, node_first,
        node_second,
    )


def solution(mesh):
    both = P(("face", "sub"))
    in_specs = (both,) * 9 + (P(None, "sub"), P("sub", None)) + (P(None, "sub", None),) * 4
    return jax.shard_map(
        per_device, mesh=mesh, in_specs=in_specs, out_specs=(both, both, P()), check_vma=False
    )
```

```python
import functools

import jax
import jax.numpy as jnp
from jax import lax
from jax.experimental import pallas as pl
from jax.experimental.pallas import tpu as pltpu
from jax.sharding import PartitionSpec as P

MESH = pl.DeviceIdType.MESH
CHUNK = 512
QUARTERED = (1, 2, 4)
BF = jnp.bfloat16
F32 = jnp.float32


def silu(v):
    return v / (1.0 + jnp.exp(-v))


def mm(a, b):
    return jnp.dot(a, b, preferred_element_type=F32)


def mm_t(a, b):
    return lax.dot_general(a, b, (((0,), (0,)), ((), ())), preferred_element_type=F32)


def hot(rows, index):
    ids = lax.broadcasted_iota(jnp.int32, (rows, index.shape[1]), 0)
    return jnp.where(ids == index, 1.0, 0.0).astype(BF)


def kernel(
    n_face, n_sub,
    mesh_hbm, edge_hbm, grid_hbm, send_hbm, recv_hbm, lists_hbm, src_hbm, dst_hbm, area_hbm,
    wg, we, w1, w2, v1, v2,
    lat_out, edge_hbm_out, mass_out,
    gg, ge, g1, g2, h1, h2,
    mesh_ref, grid_ref, send_ref, recv_ref, lists_ref, src_ref, dst_ref, area_ref,
    edges, picks, back, table, proj, halo, sums_a, sums_b, total,
    s1, r1, s2, r2, s3, r3, hs, hr, as_, ar, bs, br, ein, eout, win, pin,
):
    face, sub = lax.axis_index("face"), lax.axis_index("sub")
    core = lax.rem(face, 2)
    partner = face + 1 - 2 * core
    level = lax.rem(face // 2, 2)
    beside = face + 2 - 4 * level
    nodes, width = mesh_ref.shape
    chunks = edges.shape[0] // CHUNK

    def load_edges(i):
        rows = pl.ds(pl.multiple_of(i * CHUNK, CHUNK), CHUNK)
        return pltpu.make_async_copy(edge_hbm.at[rows], edges.at[rows], ein.at[i])

    def store_edges(i):
        rows = pl.ds(pl.multiple_of(i * CHUNK, CHUNK), CHUNK)
        return pltpu.make_async_copy(edges.at[rows], edge_hbm_out.at[rows], eout.at[i])

    shards = [wg, we, w1.at[0], w2.at[0], v1.at[0], v2.at[0]]
    wholes = [gg, ge, g1, g2, h1, h2]

    def own(w):
        rows = shards[w].shape[0]
        slot = gg.at[sub] if w == 0 else wholes[w].at[pl.ds(pl.multiple_of(sub * rows, rows), rows)]
        return pltpu.make_async_copy(shards[w], slot, win.at[w])

    pairs = [(send_hbm, send_ref), (recv_hbm, recv_ref), (src_hbm, src_ref), (dst_hbm, dst_ref),
             (grid_hbm, grid_ref), (mesh_hbm, mesh_ref), (lists_hbm, lists_ref), (area_hbm, area_ref)]
    loads = [pltpu.make_async_copy(a, b, pin.at[i]) for i, (a, b) in enumerate(pairs)]
    for w in range(6):
        own(w).start()
    for copy in loads:
        copy.start()
    for i in range(chunks):
        load_edges(i).start()

    barrier = pltpu.get_barrier_semaphore()
    for k in range(1, n_sub):
        pl.semaphore_signal(barrier, inc=1, device_id=(face, lax.rem(sub + k, n_sub)), device_id_type=MESH)
    for k in range(1, n_face):
        pl.semaphore_signal(barrier, inc=1, device_id=(lax.rem(face + k, n_face), sub), device_id_type=MESH)
    pl.semaphore_wait(barrier, n_sub + n_face - 2)

    def half_of(w, owner):
        rows = shards[w].shape[0]
        half = rows // 2
        if w == 0:
            return gg.at[owner, pl.ds(pl.multiple_of(core * half, half), half)]
        return wholes[w].at[pl.ds(pl.multiple_of(owner * rows + core * half, half), half)]

    def quarter_of(w, owner):
        rows = shards[w].shape[0]
        piece = rows // 4
        start = (core * 2 + level) * piece
        if w == 0:
            return gg.at[owner, pl.ds(pl.multiple_of(start, piece), piece)]
        return wholes[w].at[pl.ds(pl.multiple_of(owner * rows + start, piece), piece)]

    def outward(w, k):
        part = quarter_of(w, sub) if w in QUARTERED else half_of(w, sub)
        return pltpu.make_async_remote_copy(
            src_ref=part, dst_ref=part,
            send_sem=s1.at[w, k], recv_sem=r1.at[w, k],
            device_id=(face, lax.rem(sub + k, n_sub)), device_id_type=MESH)

    def upward(w, k):
        part = quarter_of(w, lax.rem(sub + n_sub - k, n_sub))
        return pltpu.make_async_remote_copy(
            src_ref=part, dst_ref=part, send_sem=s3.at[w, k], recv_sem=r3.at[w, k],
            device_id=(beside, sub), device_id_type=MESH)

    def across(w, k):
        part = half_of(w, lax.rem(sub + n_sub - k, n_sub))
        return pltpu.make_async_remote_copy(
            src_ref=part, dst_ref=part, send_sem=s2.at[w, k], recv_sem=r2.at[w, k],
            device_id=(partner, sub), device_id_type=MESH)

    def send(w):
        own(w).wait()
        for k in range(1, n_sub):
            outward(w, k).start()

    for w in range(4):
        send(w)
    for copy in loads:
        copy.wait()

    def climb(w):
        for k in range(1, n_sub):
            if w in QUARTERED:
                outward(w, k).wait_recv()
                upward(w, k).start()

    def pass_on(w):
        for k in range(1, n_sub):
            if w in QUARTERED:
                upward(w, k).wait_recv()
            else:
                outward(w, k).wait_recv()
            across(w, k).start()

    def arrive(w):
        for k in range(1, n_sub):
            across(w, k).wait_recv()

    slots = nodes + 4 * halo.shape[1]

    def mark(i, carry):
        cols = pl.ds(pl.multiple_of(i * CHUNK, CHUNK), CHUNK)
        here = hot(nodes, recv_ref[:, cols])
        back[:, cols] = here
        both = jnp.concatenate([hot(slots, send_ref[:, cols]), here], axis=0)
        picks[cols, :] = both.T
        return carry

    lax.fori_loop(0, chunks, mark, 0)
    to_node = hot(nodes, dst_ref[...])
    link_pick = jnp.concatenate([hot(grid_ref.shape[0], src_ref[...]), to_node], axis=0)

    pass_on(0)
    climb(1)
    arrive(0)
    grid = jnp.concatenate([mm(grid_ref[...], gg[j]) for j in range(n_sub)], axis=1)
    grid = silu(grid).astype(BF)
    pass_on(1)
    climb(2)
    arrive(1)
    rows = grid_ref.shape[0]
    from_grid = mm(grid, ge[:width, :]).astype(BF)
    from_mesh = mm(mesh_ref[...], ge[width:, :]).astype(BF)
    message = silu(mm_t(link_pick, jnp.concatenate([from_grid, from_mesh], axis=0))).astype(BF)
    latent = (mesh_ref[...].astype(F32) + mm(to_node, message)).astype(BF)
    table[...] = latent

    size = halo.shape[1]
    for d in range(4):
        halo[d] = mm_t(hot(nodes, lists_ref[0, d:d + 1, :]), latent).astype(BF)

    def border(d):
        step = (1, n_face - 1, 1, n_sub - 1)[d]
        to = (lax.rem(face + step, n_face), sub) if d < 2 else (face, lax.rem(sub + step, n_sub))
        return pltpu.make_async_remote_copy(
            src_ref=halo.at[d], dst_ref=halo.at[4 + d], send_sem=hs.at[d], recv_sem=hr.at[d],
            device_id=to, device_id_type=MESH)

    for d in range(4):
        border(d).start()
    send(4)
    send(5)

    pass_on(2)
    arrive(2)
    proj[:nodes, :] = mm(latent, g1[width:2 * width, :]).astype(BF)
    proj[slots:, :] = mm(latent, g1[2 * width:, :]).astype(BF)
    for d in range(4):
        border(d).wait_recv()
    outer = jnp.concatenate([halo[4 + d] for d in range(4)], axis=0)
    proj[nodes:slots, :] = mm(outer, g1[width:2 * width, :]).astype(BF)
    pass_on(3)
    arrive(3)

    total[...] = jnp.zeros_like(total)
    for i in range(chunks):
        load_edges(i).wait()

    def update(i, carry):
        cols = pl.ds(pl.multiple_of(i * CHUNK, CHUNK), CHUNK)
        edge = edges[cols, :]
        before = mm(edge, g1[:width, :]) + mm(picks[cols, :], proj[...])
        hidden = silu(before).astype(BF)
        new = (edge.astype(F32) + mm(hidden, g2[...])).astype(BF)
        edges[cols, :] = new
        total[...] += mm(back[:, cols], new)
        return carry

    lax.fori_loop(0, chunks // 2, update, 0)
    climb(4)
    lax.fori_loop(chunks // 2, chunks, update, 0)
    pass_on(4)
    pass_on(5)
    for i in range(chunks):
        store_edges(i).start()
    arrive(4)
    incoming = total[...].astype(BF)
    hidden = silu(mm(table[...], h1[:width, :]) + mm(incoming, h1[width:, :])).astype(BF)
    arrive(5)
    final = (table[...].astype(F32) + mm(hidden, h2[...])).astype(BF)
    lat_out[...] = final
    part = jnp.dot(area_ref[...], final.astype(F32), precision=lax.Precision.HIGHEST, preferred_element_type=F32)

    def share_sub(k):
        return pltpu.make_async_remote_copy(
            src_ref=sums_a.at[sub], dst_ref=sums_a.at[sub], send_sem=as_.at[k], recv_sem=ar.at[k],
            device_id=(face, lax.rem(sub + k, n_sub)), device_id_type=MESH)

    def share_face(k):
        return pltpu.make_async_remote_copy(
            src_ref=sums_b.at[face], dst_ref=sums_b.at[face], send_sem=bs.at[k], recv_sem=br.at[k],
            device_id=(lax.rem(face + k, n_face), sub), device_id_type=MESH)

    sums_a[sub] = part
    for k in range(1, n_sub):
        share_sub(k).start()
    for k in range(1, n_sub):
        share_sub(k).wait_recv()
    sums_b[face] = jnp.sum(sums_a[...], axis=0)
    for k in range(1, n_face):
        share_face(k).start()
    for k in range(1, n_face):
        share_face(k).wait_recv()
    mass_out[...] = jnp.sum(sums_b[...], axis=0) / (nodes * n_face * n_sub)

    for w in range(6):
        for k in range(1, n_sub):
            outward(w, k).wait_send()
            across(w, k).wait_send()
            if w in QUARTERED:
                upward(w, k).wait_send()
    for d in range(4):
        border(d).wait_send()
    for k in range(1, n_sub):
        share_sub(k).wait_send()
    for k in range(1, n_face):
        share_face(k).wait_send()
    for i in range(chunks):
        store_edges(i).wait()


def per_device(
    mesh_latent, edge_latent, grid_features, senders, receivers, send_lists, link_sources,
    link_targets, node_area, grid_weight, encode_weight, edge_first, edge_second, node_first,
    node_second,
):
    n_face, n_sub = lax.axis_size("face"), lax.axis_size("sub")
    nodes, width = mesh_latent.shape
    count = edge_latent.shape[0]
    size = send_lists.shape[2]
    slots = nodes + 4 * size
    chunks = count // CHUNK
    dma = pltpu.SemaphoreType.DMA
    vmem = pl.BlockSpec(memory_space=pltpu.VMEM)
    hbm = pl.BlockSpec(memory_space=pl.ANY)
    whole = [pltpu.VMEM((n_sub * w.shape[-2], width), BF)
             for w in (encode_weight, edge_first, edge_second, node_first, node_second)]
    return pl.pallas_call(
        functools.partial(kernel, n_face, n_sub),
        out_shape=(
            jax.ShapeDtypeStruct(mesh_latent.shape, BF),
            jax.ShapeDtypeStruct(edge_latent.shape, BF),
            jax.ShapeDtypeStruct((1, width), F32),
        ),
        in_specs=[hbm] * 15,
        out_specs=(vmem, hbm, vmem),
        scratch_shapes=[
            pltpu.VMEM((n_sub,) + grid_weight.shape, BF), *whole,
            pltpu.VMEM(mesh_latent.shape, BF), pltpu.VMEM(grid_features.shape, BF),
            pltpu.VMEM((1, count), jnp.int32), pltpu.VMEM((1, count), jnp.int32),
            pltpu.VMEM(send_lists.shape, jnp.int32),
            pltpu.VMEM((1, link_sources.shape[0]), jnp.int32),
            pltpu.VMEM((1, link_targets.shape[0]), jnp.int32),
            pltpu.VMEM((1, nodes), F32),
            pltpu.VMEM(edge_latent.shape, BF),
            pltpu.VMEM((count, slots + nodes), BF),
            pltpu.VMEM((nodes, count), BF),
            pltpu.VMEM((nodes, width), BF),
            pltpu.VMEM((slots + nodes, width), BF),
            pltpu.VMEM((8, size, width), BF),
            pltpu.VMEM((n_sub, 1, width), F32),
            pltpu.VMEM((n_face, 1, width), F32),
            pltpu.VMEM((nodes, width), F32),
            *[dma((6, n_sub))] * 6,
            dma((4,)), dma((4,)), dma((n_sub,)), dma((n_sub,)), dma((n_face,)), dma((n_face,)),
            dma((chunks,)), dma((chunks,)), dma((6,)), dma((8,)),
        ],
        compiler_params=pltpu.CompilerParams(
            collective_id=0, has_side_effects=True, vmem_limit_bytes=67043328
        ),
    )(
        mesh_latent, edge_latent, grid_features, senders.reshape(1, -1), receivers.reshape(1, -1),
        send_lists, link_sources.reshape(1, -1), link_targets.reshape(1, -1),
        node_area.reshape(1, -1), grid_weight, encode_weight, edge_first, edge_second, node_first,
        node_second,
    )


def solution(mesh):
    both = P(("face", "sub"))
    in_specs = (both,) * 9 + (P(None, "sub"), P("sub", None)) + (P(None, "sub", None),) * 4
    return jax.shard_map(
        per_device, mesh=mesh, in_specs=in_specs, out_specs=(both, both, P()), check_vma=False
    )
```

```python
import functools

import jax
import jax.numpy as jnp
from jax import lax
from jax.experimental import pallas as pl
from jax.experimental.pallas import tpu as pltpu
from jax.sharding import PartitionSpec as P

MESH = pl.DeviceIdType.MESH
CHUNK = 512
QUARTERED = (1, 2)
BF = jnp.bfloat16
F32 = jnp.float32


def silu(v):
    return v / (1.0 + jnp.exp(-v))


def mm(a, b):
    return jnp.dot(a, b, preferred_element_type=F32)


def mm_t(a, b):
    return lax.dot_general(a, b, (((0,), (0,)), ((), ())), preferred_element_type=F32)


def hot(rows, index):
    ids = lax.broadcasted_iota(jnp.int32, (rows, index.shape[1]), 0)
    return jnp.where(ids == index, 1.0, 0.0).astype(BF)


def kernel(
    n_face, n_sub,
    mesh_hbm, edge_hbm, grid_hbm, send_hbm, recv_hbm, lists_hbm, src_hbm, dst_hbm, area_hbm,
    wg, we, w1, w2, v1, v2,
    lat_out, edge_hbm_out, mass_out,
    gg, ge, g1, g2, h1, h2,
    mesh_ref, grid_ref, send_ref, recv_ref, lists_ref, src_ref, dst_ref, area_ref,
    edges, picks, back, table, proj, halo, sums_a, sums_b, total,
    s1, r1, s2, r2, s3, r3, hs, hr, as_, ar, bs, br, ein, eout, win, pin,
):
    face, sub = lax.axis_index("face"), lax.axis_index("sub")
    core = lax.rem(face, 2)
    partner = face + 1 - 2 * core
    level = lax.rem(face // 2, 2)
    beside = face + 2 - 4 * level
    nodes, width = mesh_ref.shape
    chunks = edges.shape[0] // CHUNK

    def load_edges(i):
        rows = pl.ds(pl.multiple_of(i * CHUNK, CHUNK), CHUNK)
        return pltpu.make_async_copy(edge_hbm.at[rows], edges.at[rows], ein.at[i])

    def store_edges(i):
        rows = pl.ds(pl.multiple_of(i * CHUNK, CHUNK), CHUNK)
        return pltpu.make_async_copy(edges.at[rows], edge_hbm_out.at[rows], eout.at[i])

    shards = [wg, we, w1.at[0], w2.at[0], v1.at[0], v2.at[0]]
    wholes = [gg, ge, g1, g2, h1, h2]

    def own(w):
        rows = shards[w].shape[0]
        slot = gg.at[sub] if w == 0 else wholes[w].at[pl.ds(pl.multiple_of(sub * rows, rows), rows)]
        return pltpu.make_async_copy(shards[w], slot, win.at[w])

    pairs = [(send_hbm, send_ref), (recv_hbm, recv_ref), (src_hbm, src_ref), (dst_hbm, dst_ref),
             (grid_hbm, grid_ref), (mesh_hbm, mesh_ref), (lists_hbm, lists_ref), (area_hbm, area_ref)]
    loads = [pltpu.make_async_copy(a, b, pin.at[i]) for i, (a, b) in enumerate(pairs)]
    for w in range(6):
        own(w).start()
    for copy in loads:
        copy.start()
    for i in range(chunks):
        load_edges(i).start()

    barrier = pltpu.get_barrier_semaphore()
    for k in range(1, n_sub):
        pl.semaphore_signal(barrier, inc=1, device_id=(face, lax.rem(sub + k, n_sub)), device_id_type=MESH)
    for k in range(1, n_face):
        pl.semaphore_signal(barrier, inc=1, device_id=(lax.rem(face + k, n_face), sub), device_id_type=MESH)
    pl.semaphore_wait(barrier, n_sub + n_face - 2)

    def half_of(w, owner):
        rows = shards[w].shape[0]
        half = rows // 2
        if w == 0:
            return gg.at[owner, pl.ds(pl.multiple_of(core * half, half), half)]
        return wholes[w].at[pl.ds(pl.multiple_of(owner * rows + core * half, half), half)]

    def quarter_of(w, owner):
        rows = shards[w].shape[0]
        piece = rows // 4
        start = (core * 2 + level) * piece
        if w == 0:
            return gg.at[owner, pl.ds(pl.multiple_of(start, piece), piece)]
        return wholes[w].at[pl.ds(pl.multiple_of(owner * rows + start, piece), piece)]

    def outward(w, k):
        part = quarter_of(w, sub) if w in QUARTERED else half_of(w, sub)
        return pltpu.make_async_remote_copy(
            src_ref=part, dst_ref=part,
            send_sem=s1.at[w, k], recv_sem=r1.at[w, k],
            device_id=(face, lax.rem(sub + k, n_sub)), device_id_type=MESH)

    def upward(w, k):
        part = quarter_of(w, lax.rem(sub + n_sub - k, n_sub))
        return pltpu.make_async_remote_copy(
            src_ref=part, dst_ref=part, send_sem=s3.at[w, k], recv_sem=r3.at[w, k],
            device_id=(beside, sub), device_id_type=MESH)

    def across(w, k):
        part = half_of(w, lax.rem(sub + n_sub - k, n_sub))
        return pltpu.make_async_remote_copy(
            src_ref=part, dst_ref=part, send_sem=s2.at[w, k], recv_sem=r2.at[w, k],
            device_id=(partner, sub), device_id_type=MESH)

    def send(w):
        own(w).wait()
        for k in range(1, n_sub):
            outward(w, k).start()

    for w in range(4):
        send(w)
    for copy in loads:
        copy.wait()

    def climb(w):
        for k in range(1, n_sub):
            if w in QUARTERED:
                outward(w, k).wait_recv()
                upward(w, k).start()

    def pass_on(w):
        for k in range(1, n_sub):
            if w in QUARTERED:
                upward(w, k).wait_recv()
            else:
                outward(w, k).wait_recv()
            across(w, k).start()

    def arrive(w):
        for k in range(1, n_sub):
            across(w, k).wait_recv()

    slots = nodes + 4 * halo.shape[1]

    def mark(i, carry):
        cols = pl.ds(pl.multiple_of(i * CHUNK, CHUNK), CHUNK)
        here = hot(nodes, recv_ref[:, cols])
        back[:, cols] = here
        both = jnp.concatenate([hot(slots, send_ref[:, cols]), here], axis=0)
        picks[cols, :] = both.T
        return carry

    lax.fori_loop(0, chunks, mark, 0)
    to_node = hot(nodes, dst_ref[...])
    link_pick = jnp.concatenate([hot(grid_ref.shape[0], src_ref[...]), to_node], axis=0)

    pass_on(0)
    climb(1)
    arrive(0)
    grid = jnp.concatenate([mm(grid_ref[...], gg[j]) for j in range(n_sub)], axis=1)
    grid = silu(grid).astype(BF)
    pass_on(1)
    climb(2)
    arrive(1)
    rows = grid_ref.shape[0]
    from_grid = mm(grid, ge[:width, :]).astype(BF)
    from_mesh = mm(mesh_ref[...], ge[width:, :]).astype(BF)
    message = silu(mm_t(link_pick, jnp.concatenate([from_grid, from_mesh], axis=0))).astype(BF)
    latent = (mesh_ref[...].astype(F32) + mm(to_node, message)).astype(BF)
    table[...] = latent

    size = halo.shape[1]
    for d in range(4):
        halo[d] = mm_t(hot(nodes, lists_ref[0, d:d + 1, :]), latent).astype(BF)

    def border(d):
        step = (1, n_face - 1, 1, n_sub - 1)[d]
        to = (lax.rem(face + step, n_face), sub) if d < 2 else (face, lax.rem(sub + step, n_sub))
        return pltpu.make_async_remote_copy(
            src_ref=halo.at[d], dst_ref=halo.at[4 + d], send_sem=hs.at[d], recv_sem=hr.at[d],
            device_id=to, device_id_type=MESH)

    for d in range(4):
        border(d).start()
    send(4)
    send(5)

    pass_on(2)
    arrive(2)
    proj[:nodes, :] = mm(latent, g1[width:2 * width, :]).astype(BF)
    proj[slots:, :] = mm(latent, g1[2 * width:, :]).astype(BF)
    for d in range(4):
        border(d).wait_recv()
    outer = jnp.concatenate([halo[4 + d] for d in range(4)], axis=0)
    proj[nodes:slots, :] = mm(outer, g1[width:2 * width, :]).astype(BF)
    pass_on(3)
    arrive(3)

    total[...] = jnp.zeros_like(total)
    for i in range(chunks):
        load_edges(i).wait()

    def update(i, carry):
        cols = pl.ds(pl.multiple_of(i * CHUNK, CHUNK), CHUNK)
        edge = edges[cols, :]
        before = mm(edge, g1[:width, :]) + mm(picks[cols, :], proj[...])
        hidden = silu(before).astype(BF)
        new = (edge.astype(F32) + mm(hidden, g2[...])).astype(BF)
        edges[cols, :] = new
        total[...] += mm(back[:, cols], new)
        return carry

    lax.fori_loop(0, chunks // 2, update, 0)
    climb(4)
    lax.fori_loop(chunks // 2, chunks, update, 0)
    pass_on(4)
    pass_on(5)
    for i in range(chunks):
        store_edges(i).start()
    arrive(4)
    incoming = total[...].astype(BF)
    hidden = silu(mm(table[...], h1[:width, :]) + mm(incoming, h1[width:, :])).astype(BF)
    arrive(5)
    final = (table[...].astype(F32) + mm(hidden, h2[...])).astype(BF)
    lat_out[...] = final
    part = jnp.dot(area_ref[...], final.astype(F32), precision=lax.Precision.HIGHEST, preferred_element_type=F32)

    def share_sub(k):
        return pltpu.make_async_remote_copy(
            src_ref=sums_a.at[sub], dst_ref=sums_a.at[sub], send_sem=as_.at[k], recv_sem=ar.at[k],
            device_id=(face, lax.rem(sub + k, n_sub)), device_id_type=MESH)

    def share_face(k):
        return pltpu.make_async_remote_copy(
            src_ref=sums_b.at[face], dst_ref=sums_b.at[face], send_sem=bs.at[k], recv_sem=br.at[k],
            device_id=(lax.rem(face + k, n_face), sub), device_id_type=MESH)

    sums_a[sub] = part
    for k in range(1, n_sub):
        share_sub(k).start()
    for k in range(1, n_sub):
        share_sub(k).wait_recv()
    sums_b[face] = jnp.sum(sums_a[...], axis=0)
    for k in range(1, n_face):
        share_face(k).start()
    for k in range(1, n_face):
        share_face(k).wait_recv()
    mass_out[...] = jnp.sum(sums_b[...], axis=0) / (nodes * n_face * n_sub)

    for w in range(6):
        for k in range(1, n_sub):
            outward(w, k).wait_send()
            across(w, k).wait_send()
            if w in QUARTERED:
                upward(w, k).wait_send()
    for d in range(4):
        border(d).wait_send()
    for k in range(1, n_sub):
        share_sub(k).wait_send()
    for k in range(1, n_face):
        share_face(k).wait_send()
    for i in range(chunks):
        store_edges(i).wait()


def per_device(
    mesh_latent, edge_latent, grid_features, senders, receivers, send_lists, link_sources,
    link_targets, node_area, grid_weight, encode_weight, edge_first, edge_second, node_first,
    node_second,
):
    n_face, n_sub = lax.axis_size("face"), lax.axis_size("sub")
    nodes, width = mesh_latent.shape
    count = edge_latent.shape[0]
    size = send_lists.shape[2]
    slots = nodes + 4 * size
    chunks = count // CHUNK
    dma = pltpu.SemaphoreType.DMA
    vmem = pl.BlockSpec(memory_space=pltpu.VMEM)
    hbm = pl.BlockSpec(memory_space=pl.ANY)
    whole = [pltpu.VMEM((n_sub * w.shape[-2], width), BF)
             for w in (encode_weight, edge_first, edge_second, node_first, node_second)]
    return pl.pallas_call(
        functools.partial(kernel, n_face, n_sub),
        out_shape=(
            jax.ShapeDtypeStruct(mesh_latent.shape, BF),
            jax.ShapeDtypeStruct(edge_latent.shape, BF),
            jax.ShapeDtypeStruct((1, width), F32),
        ),
        in_specs=[hbm] * 15,
        out_specs=(vmem, hbm, vmem),
        scratch_shapes=[
            pltpu.VMEM((n_sub,) + grid_weight.shape, BF), *whole,
            pltpu.VMEM(mesh_latent.shape, BF), pltpu.VMEM(grid_features.shape, BF),
            pltpu.VMEM((1, count), jnp.int32), pltpu.VMEM((1, count), jnp.int32),
            pltpu.VMEM(send_lists.shape, jnp.int32),
            pltpu.VMEM((1, link_sources.shape[0]), jnp.int32),
            pltpu.VMEM((1, link_targets.shape[0]), jnp.int32),
            pltpu.VMEM((1, nodes), F32),
            pltpu.VMEM(edge_latent.shape, BF),
            pltpu.VMEM((count, slots + nodes), BF),
            pltpu.VMEM((nodes, count), BF),
            pltpu.VMEM((nodes, width), BF),
            pltpu.VMEM((slots + nodes, width), BF),
            pltpu.VMEM((8, size, width), BF),
            pltpu.VMEM((n_sub, 1, width), F32),
            pltpu.VMEM((n_face, 1, width), F32),
            pltpu.VMEM((nodes, width), F32),
            *[dma((6, n_sub))] * 6,
            dma((4,)), dma((4,)), dma((n_sub,)), dma((n_sub,)), dma((n_face,)), dma((n_face,)),
            dma((chunks,)), dma((chunks,)), dma((6,)), dma((8,)),
        ],
        compiler_params=pltpu.CompilerParams(
            collective_id=0, has_side_effects=True, vmem_limit_bytes=67043328
        ),
    )(
        mesh_latent, edge_latent, grid_features, senders.reshape(1, -1), receivers.reshape(1, -1),
        send_lists, link_sources.reshape(1, -1), link_targets.reshape(1, -1),
        node_area.reshape(1, -1), grid_weight, encode_weight, edge_first, edge_second, node_first,
        node_second,
    )


def solution(mesh):
    both = P(("face", "sub"))
    in_specs = (both,) * 9 + (P(None, "sub"), P("sub", None)) + (P(None, "sub", None),) * 4
    return jax.shard_map(
        per_device, mesh=mesh, in_specs=in_specs, out_specs=(both, both, P()), check_vma=False
    )
```
